32 devices in a mesh: cp: 32 (over z, y, x, core).
Axes of the slice: x: 2, y: 2, z: 4, core: 2. Of those that a mesh axis runs over, the one named last changes fastest.
Arguments:
- x_in_a: bfloat16 [1, 4096, 1024], P(None, 'cp')
- x_in_b: bfloat16 [1, 4096, 1024], P(None, 'cp')
- dy_out_a: bfloat16 [1, 4096, 1024], P(None, 'cp')
- dy_out_b: bfloat16 [1, 4096, 1024], P(None, 'cp')
- gain_in_a: bfloat16 [1024], replicated
- gain_in_b: bfloat16 [1024], replicated
- w_qa: bfloat16 [1024, 2048], replicated
- w_qb: bfloat16 [1024, 2048], replicated
- w_k: bfloat16 [1024, 1024], replicated
- w_v: bfloat16 [1024, 1024], replicated
- w_oa: bfloat16 [2048, 1024], replicated
- w_ob: bfloat16 [2048, 1024], replicated
- gain_qa: bfloat16 [128], replicated
- gain_qb: bfloat16 [128], replicated
- gain_k: bfloat16 [128], replicated
Outputs:
- output 1: bfloat16 [1, 4096, 1024], P(None, 'cp')
- output 2: bfloat16 [1, 4096, 1024], P(None, 'cp')
- output 3: bfloat16 [1, 4096, 1024], P(None, 'cp')
- output 4: bfloat16 [1, 4096, 1024], P(None, 'cp')
- output 5: float32 [1024, 2048], replicated
- output 6: float32 [1024, 2048], replicated
- output 7: float32 [1024, 1024], replicated
- output 8: float32 [1024, 1024], replicated
- output 9: float32 [2048, 1024], replicated
- output 10: float32 [2048, 1024], replicated
All inputs are finite; a program needn't handle non-finite values.
Results may differ from the reference program's by a relative error of at most 0.0139066.
Values are sent between devices in bfloat16 or wider.
A program may use at most 1 GiB of HBM per device.

```python
import functools
import jax
import jax.numpy as jnp
from jax import lax

D_MODEL = 1024
N_HEADS = 16
KV_HEADS = 8
HEAD_DIM = 128
N_BATCH = 1
TOK_DEV = 128
CP_SIZE = 32
Q_BLOCK = 16

SEQ_LEN = TOK_DEV * CP_SIZE
PIECE_LEN = TOK_DEV // 2
GROUPS = N_HEADS // KV_HEADS
Q_WIDTH = N_HEADS * HEAD_DIM
KV_WIDTH = KV_HEADS * HEAD_DIM


def setup_inputs(seed: int = 0) -> dict:
    key_list = jax.random.split(jax.random.key(seed), 15)
    act_shape = (N_BATCH, SEQ_LEN, D_MODEL)

    def draw_arr(key_idx, arr_shape, spread, offset):
        noise_arr = jax.random.normal(key_list[key_idx], arr_shape, jnp.float32)
        return (offset + spread * noise_arr).astype(jnp.bfloat16)

    return {
        'x_in_a': draw_arr(0, act_shape, 1.0, 0.0),
        'x_in_b': draw_arr(1, act_shape, 1.0, 0.0),
        'dy_out_a': draw_arr(2, act_shape, 1.0, 0.0),
        'dy_out_b': draw_arr(3, act_shape, 1.0, 0.0),
        'gain_in_a': draw_arr(4, (D_MODEL,), 0.3, 1.0),
        'gain_in_b': draw_arr(5, (D_MODEL,), 0.3, 1.0),
        'w_qa': draw_arr(6, (D_MODEL, Q_WIDTH), D_MODEL ** -0.5, 0.0),
        'w_qb': draw_arr(7, (D_MODEL, Q_WIDTH), D_MODEL ** -0.5, 0.0),
        'w_k': draw_arr(8, (D_MODEL, KV_WIDTH), D_MODEL ** -0.5, 0.0),
        'w_v': draw_arr(9, (D_MODEL, KV_WIDTH), D_MODEL ** -0.5, 0.0),
        'w_oa': draw_arr(10, (Q_WIDTH, D_MODEL), Q_WIDTH ** -0.5, 0.0),
        'w_ob': draw_arr(11, (Q_WIDTH, D_MODEL), Q_WIDTH ** -0.5, 0.0),
        'gain_qa': draw_arr(12, (HEAD_DIM,), 0.3, 1.0),
        'gain_qb': draw_arr(13, (HEAD_DIM,), 0.3, 1.0),
        'gain_k': draw_arr(14, (HEAD_DIM,), 0.3, 1.0),
    }


def to_bf16_grid(values):
    return values + lax.stop_gradient(values.astype(jnp.bfloat16).astype(jnp.float32) - values)


def rms_norm(values, gain_vec):
    inv_rms = lax.rsqrt(jnp.mean(values * values, axis=-1, keepdims=True) + 1e-6)
    return values * inv_rms * gain_vec


def rotary(values, positions):
    half_dim = HEAD_DIM // 2
    inv_freq = 10000.0 ** (-jnp.arange(half_dim, dtype=jnp.float32) / half_dim)
    angles = positions.astype(jnp.float32)[:, None] * inv_freq[None, :]
    bshape = (1, positions.shape[0]) + (1,) * (values.ndim - 3) + (half_dim,)
    cos_vals = jnp.cos(angles).reshape(bshape)
    sine_vals = jnp.sin(angles).reshape(bshape)
    first_half = values[..., :half_dim]
    second_half = values[..., half_dim:]
    return jnp.concatenate([first_half * cos_vals - second_half * sine_vals, second_half * cos_vals + first_half * sine_vals], axis=-1)


def stored_positions():
    row_idx = jnp.arange(SEQ_LEN)
    owner_dev = row_idx // TOK_DEV
    within = row_idx % TOK_DEV
    return jnp.where(within < PIECE_LEN, owner_dev * PIECE_LEN + within, (2 * CP_SIZE - 1 - owner_dev) * PIECE_LEN + within - PIECE_LEN)


def attention(queries, keys_all, vals_all, positions):
    n_blocks = SEQ_LEN // Q_BLOCK
    q_blocks = jnp.moveaxis(queries.reshape(N_BATCH, n_blocks, Q_BLOCK, KV_HEADS, 2 * GROUPS, HEAD_DIM), 1, 0)
    pos_blocks = positions.reshape(n_blocks, Q_BLOCK)

    def one_block(block_in):
        q_blk, pos_blk = block_in
        scores = jnp.einsum('bqhgd,bkhd->bhgqk', q_blk, keys_all) * HEAD_DIM ** -0.5
        causal_mask = positions[None, :] <= pos_blk[:, None]
        weights = to_bf16_grid(jax.nn.softmax(jnp.where(causal_mask, scores, -1e30), axis=-1))
        return jnp.einsum('bhgqk,bkhd->bqhgd', weights, vals_all)

    out_blocks = lax.map(jax.checkpoint(one_block), (q_blocks, pos_blocks))
    return jnp.moveaxis(out_blocks, 0, 1).reshape(N_BATCH, SEQ_LEN, KV_HEADS, 2 * GROUPS, HEAD_DIM)


def forward(x_in_a, x_in_b, w_qa, w_qb, w_k, w_v, w_oa, w_ob, gains):
    gain_in_a, gain_in_b, gain_qa, gain_qb, gain_k = gains
    positions = stored_positions()
    normed_a = to_bf16_grid(rms_norm(x_in_a, gain_in_a))
    normed_b = to_bf16_grid(rms_norm(x_in_b, gain_in_b))
    q_shape = (N_BATCH, SEQ_LEN, KV_HEADS, GROUPS, HEAD_DIM)
    kv_shape = (N_BATCH, SEQ_LEN, KV_HEADS, HEAD_DIM)
    query_a = to_bf16_grid(rotary(rms_norm(jnp.einsum('btd,de->bte', normed_a, w_qa).reshape(q_shape), gain_qa), positions))
    query_b = to_bf16_grid(rotary(rms_norm(jnp.einsum('btd,de->bte', normed_b, w_qb).reshape(q_shape), gain_qb), positions))
    keys_all = to_bf16_grid(rotary(rms_norm(jnp.einsum('btd,de->bte', normed_a, w_k).reshape(kv_shape), gain_k), positions))
    vals_all = to_bf16_grid(jnp.einsum('btd,de->bte', normed_a, w_v)).reshape(kv_shape)
    attn_out = to_bf16_grid(attention(jnp.concatenate([query_a, query_b], axis=3), keys_all, vals_all, positions))
    out_a = attn_out[:, :, :, :GROUPS, :].reshape(N_BATCH, SEQ_LEN, Q_WIDTH)
    out_b = attn_out[:, :, :, GROUPS:, :].reshape(N_BATCH, SEQ_LEN, Q_WIDTH)
    y_out_a = x_in_a + jnp.einsum('bte,ed->btd', out_a, w_oa)
    y_out_b = x_in_b + jnp.einsum('bte,ed->btd', out_b, w_ob)
    return y_out_a, y_out_b


def reference(x_in_a, x_in_b, dy_out_a, dy_out_b, gain_in_a, gain_in_b, w_qa, w_qb, w_k, w_v, w_oa, w_ob, gain_qa, gain_qb, gain_k):
    gains = tuple(arr_val.astype(jnp.float32) for arr_val in (gain_in_a, gain_in_b, gain_qa, gain_qb, gain_k))
    primals = [arr_val.astype(jnp.float32) for arr_val in (x_in_a, x_in_b, w_qa, w_qb, w_k, w_v, w_oa, w_ob)]
    outputs, pullback = jax.vjp(functools.partial(forward, gains=gains), *primals)
    grad_list = pullback((dy_out_a.astype(jnp.float32), dy_out_b.astype(jnp.float32)))
    return (outputs[0].astype(jnp.bfloat16), outputs[1].astype(jnp.bfloat16), grad_list[0].astype(jnp.bfloat16), grad_list[1].astype(jnp.bfloat16), grad_list[2], grad_list[3], grad_list[4], grad_list[5], grad_list[6], grad_list[7])
```

```python
import functools
import jax
import jax.numpy as jnp
from jax import lax
from jax.experimental import pallas as pl
from jax.experimental.pallas import tpu as pltpu
from jax.sharding import PartitionSpec as P

EPSILON = 1e-6
ROPE_BASE = 10000.0
NEG_BIG = -1e30
LOG2E = 1.4426950408889634
F32 = jnp.float32
BF16 = jnp.bfloat16
HD, DM, SEQ, BLK, PC, HALF, ND, NB, NG = 128, 1024, 4096, 512, 64, 2048, 32, 8, 4
VMEM_LIMIT = 58 * 1024 * 1024


def rms_norm(values, gain_vec):
    vals32 = values.astype(F32)
    inv_rms = lax.rsqrt(jnp.mean(vals32 * vals32, axis=-1, keepdims=True) + EPSILON)
    return vals32 * inv_rms * gain_vec.astype(F32)


def head_norm_rope(proj, gain, cos_full, sin_full):
    inv = lax.rsqrt(jnp.mean(proj * proj, axis=-1, keepdims=True) + EPSILON)
    normed = proj * inv * gain
    return normed * cos_full + jnp.concatenate([normed[:, PC:], normed[:, :PC]], axis=-1) * sin_full


def head_norm_rope_vjp(grad, proj, gain, cos_full, sin_full):
    gs = grad * sin_full
    dn = (grad * cos_full + jnp.concatenate([gs[:, PC:], gs[:, :PC]], axis=-1)) * gain
    inv = lax.rsqrt(jnp.mean(proj * proj, axis=-1, keepdims=True) + EPSILON)
    xhat = proj * inv
    return inv * (dn - xhat * jnp.mean(dn * xhat, axis=-1, keepdims=True))


def dot(a, b, ca, cb):
    return lax.dot_general(a, b, (((ca,), (cb,)), ((), ())), preferred_element_type=F32)


def piece_row(dev, half):
    return pl.multiple_of((dev if half == 0 else 63 - dev) * PC, PC)


def proj_kernel(idx_ref, hl_ref, ha_ref, wq_ref, wkv_ref, gq_ref, gk_ref, cos_ref, sin_ref,
                q_ref, k_ref, v_ref, qp_ref, kp_ref):
    t = pl.program_id(0)
    qp = dot(hl_ref[...].reshape(BLK, DM), wq_ref[...], 1, 0)
    kvp = dot(ha_ref[...].reshape(BLK, DM), wkv_ref[...], 1, 0)
    for u in range(NG):
        for half in range(2):
            rows = slice(u * HD + half * PC, u * HD + half * PC + PC)
            dst = pl.ds(piece_row(t * NG + u, half), PC)
            cos_p, sin_p = cos_ref[dst, :], sin_ref[dst, :]
            qp_ref[dst, :] = qp[rows]
            kp_ref[dst, :] = kvp[rows, :HD]
            q_ref[dst, :] = head_norm_rope(qp[rows], gq_ref[...], cos_p, sin_p).astype(BF16)
            k_ref[dst, :] = head_norm_rope(kvp[rows, :HD], gk_ref[...], cos_p, sin_p).astype(BF16)
            v_ref[dst, :] = kvp[rows, HD:].astype(BF16)


def dout_kernel(idx_ref, dy_ref, wo_ref, do_ref):
    t = pl.program_id(0)
    d_out = dot(dy_ref[...].reshape(BLK, DM), wo_ref[...], 1, 1).astype(BF16)
    for u in range(NG):
        for half in range(2):
            rows = slice(u * HD + half * PC, u * HD + half * PC + PC)
            do_ref[pl.ds(piece_row(t * NG + u, half), PC), :] = d_out[rows]


def store_pieces(ref, block, blk_idx, count):
    for u in range(count):
        piece = blk_idx * count + u
        rows = block[u * PC:(u + 1) * PC]

        @pl.when(piece < ND)
        def _():
            ref[piece, 0:PC, :] = rows

        @pl.when(piece >= ND)
        def _():
            ref[63 - piece, PC:HD, :] = rows


def fwd_kernel(q_ref, k_ref, v_ref, o_ref, lse_ref, acc_ref, *, scale):
    i = pl.program_id(0)
    q = q_ref[...]
    c2 = scale * LOG2E

    def step(j, carry, masked):
        m, l = carry
        rows = pl.ds(pl.multiple_of(j * BLK, BLK), BLK)
        s = dot(k_ref[rows, :], q, 1, 1)
        if masked:
            kid = lax.broadcasted_iota(jnp.int32, (BLK, BLK), 0)
            qid = lax.broadcasted_iota(jnp.int32, (BLK, BLK), 1)
            s = jnp.where(kid <= qid, s, NEG_BIG)
        m_new = jnp.maximum(m, jnp.max(s, axis=0, keepdims=True))
        p = jnp.exp2((s - m_new) * c2)
        alpha = jnp.exp2((m - m_new) * c2)
        l_new = l * alpha + jnp.sum(p, axis=0, keepdims=True)
        acc_ref[...] = acc_ref[...] * alpha + dot(v_ref[rows, :], p.astype(BF16), 0, 0)
        return m_new, l_new

    acc_ref[...] = jnp.zeros_like(acc_ref)
    init = (jnp.full((1, BLK), NEG_BIG, F32), jnp.zeros((1, BLK), F32))
    m, l = step(i, init, True)
    m, l = lax.fori_loop(0, i, lambda j, cr: step(j, cr, False), (m, l))
    lse_ref[i] = m * scale + jnp.log(l)
    o_blk = (acc_ref[...] / l).T.astype(BF16)
    store_pieces(o_ref, o_blk, i, NB)


def bwd_kernel(idx_ref, q_ref, k_ref, v_ref, do_ref, o_ref, lse_ref, qp_ref, gq_ref, cos_ref, sin_ref,
               dq_ref, dkv_ref, dqt_ref, dk_acc, dv_acc, delta_ref, *, scale):
    j = pl.program_id(0)
    layer, core = idx_ref[0], idx_ref[1]
    k = k_ref[...]
    v = v_ref[...]
    c2 = scale * LOG2E

    @pl.when(j == 0)
    def _():
        dqt_ref[...] = jnp.zeros_like(dqt_ref)
        for i in range(NB):
            parts = []
            for u in range(NB):
                piece = i * NB + u
                if piece < ND:
                    parts.append(o_ref[piece, 0:PC, :])
                else:
                    parts.append(o_ref[63 - piece, PC:HD, :])
            o_blk = jnp.concatenate(parts, axis=0).astype(F32)
            prod = o_blk * do_ref[i * BLK:(i + 1) * BLK, :].astype(F32)
            delta_ref[i] = jnp.sum(prod.T, axis=0, keepdims=True)

    dk_acc[...] = jnp.zeros_like(dk_acc)
    dv_acc[...] = jnp.zeros_like(dv_acc)

    def step(i, masked):
        rows = pl.ds(pl.multiple_of(i * BLK, BLK), BLK)
        q = q_ref[rows, :]
        do = do_ref[rows, :]
        s = dot(k, q, 1, 1)
        p = jnp.exp2(s * c2 - lse_ref[i] * LOG2E)
        if masked:
            kid = lax.broadcasted_iota(jnp.int32, (BLK, BLK), 0)
            qid = lax.broadcasted_iota(jnp.int32, (BLK, BLK), 1)
            p = jnp.where(kid <= qid, p, 0.0)
        dp = dot(v, do, 1, 1)
        ds = (p * (dp - delta_ref[i]) * scale).astype(BF16)
        dv_acc[...] += dot(p.astype(BF16), do, 1, 0)
        dk_acc[...] += dot(ds, q, 1, 0)
        dqt_ref[i] += dot(k, ds, 0, 0)

    step(j, True)

    @pl.loop(j + 1, NB)
    def _(i):
        step(i, False)

    pos = jnp.where(j // NG == layer, 0, 1)
    rows = pl.ds(pl.multiple_of((j % NG) * BLK, BLK), BLK)
    dkv_ref[core, pos, rows, :] = dk_acc[...]
    dkv_ref[1 - core, pos, rows, :] = dv_acc[...]

    rows_q = pl.ds(pl.multiple_of(j * BLK, BLK), BLK)
    dq = dqt_ref[j].T
    d_proj = head_norm_rope_vjp(dq, qp_ref[rows_q, :], gq_ref[...], cos_ref[rows_q, :], sin_ref[rows_q, :])
    store_pieces(dq_ref, d_proj.astype(BF16), j, NB)


def dwo_kernel(idx_ref, o_ref, dy_ref, out_ref):
    @pl.when(pl.program_id(0) == 0)
    def _():
        out_ref[...] = jnp.zeros_like(out_ref)

    out_ref[...] += dot(o_ref[...].reshape(BLK, HD), dy_ref[...].reshape(BLK, DM), 0, 0)


def dwq_kernel(idx_ref, h_ref, d_ref, out_ref, acc_ref):
    t = pl.program_id(0)

    @pl.when(t == 0)
    def _():
        acc_ref[...] = jnp.zeros_like(acc_ref)

    acc_ref[...] += dot(d_ref[...].reshape(BLK, HD), h_ref[...].reshape(BLK, acc_ref.shape[1]), 0, 0)

    @pl.when(t == pl.num_programs(0) - 1)
    def _():
        out_ref[...] = acc_ref[...].T


def full(shape):
    return pl.BlockSpec(shape, lambda t, *_: (0,) * len(shape), pipeline_mode=pl.Buffered(1))


def full_out(shape):
    return pl.BlockSpec(shape, lambda t, *_: (0,) * len(shape))


def call(body, name, grid, in_specs, out_specs, out_shape, flops, scratch=(), prefetch=1):
    return pl.pallas_call(
        body, name=name, out_shape=out_shape,
        grid_spec=pltpu.PrefetchScalarGridSpec(
            num_scalar_prefetch=prefetch, grid=grid, in_specs=in_specs, out_specs=out_specs,
            scratch_shapes=list(scratch)),
        compiler_params=pltpu.CompilerParams(
            dimension_semantics=("arbitrary",), vmem_limit_bytes=VMEM_LIMIT),
        cost_estimate=pl.CostEstimate(flops=int(flops), bytes_accessed=1 << 23, transcendentals=0))


def solution(mesh):
    act_spec = P(None, 'cp', None)
    rep_spec = P()
    ndev = mesh.shape['cp']
    core_perm = [(s, s ^ 1) for s in range(ndev)]
    layer_perm = [(s, s ^ 2) for s in range(ndev)]

    def local_fn(x_in_a, x_in_b, dy_out_a, dy_out_b, gain_in_a, gain_in_b, w_qa, w_qb, w_k, w_v, w_oa, w_ob, gain_qa, gain_qb, gain_k):
        scale = HD ** -0.5
        rank = lax.axis_index('cp')
        grp, layer, core = rank // NG, (rank // 2) % 2, rank % 2
        head = 2 * grp + core
        is_a = layer == 0
        idx = jnp.stack([layer, core]).astype(jnp.int32)

        h_loc = jnp.stack([rms_norm(x_in_a[0], gain_in_a).astype(BF16), rms_norm(x_in_b[0], gain_in_b).astype(BF16)])
        h_all = lax.all_gather(h_loc, 'cp')
        dy_loc, h_all = lax.optimization_barrier((jnp.stack([dy_out_a[0], dy_out_b[0]]), h_all))
        dy_all = lax.all_gather(dy_loc, 'cp')

        def cols(w, at):
            return lax.dynamic_slice(w, (0, at * HD), (w.shape[0], HD))

        wq = jnp.where(is_a, cols(w_qa, head), cols(w_qb, head))
        wkv = jnp.concatenate([cols(w_k, grp), cols(w_v, grp)], axis=1)
        wo = jnp.where(is_a, lax.dynamic_slice(w_oa, (head * HD, 0), (HD, DM)),
                       lax.dynamic_slice(w_ob, (head * HD, 0), (HD, DM)))
        gq = jnp.where(is_a, gain_qa, gain_qb).astype(F32).reshape(1, HD)
        gk = gain_k.astype(F32).reshape(1, HD)
        inv_freq = ROPE_BASE ** (-jnp.arange(PC, dtype=F32) / PC)
        angles = jnp.arange(SEQ, dtype=F32)[:, None] * inv_freq[None, :]
        cos_h, sin_h = jnp.cos(angles), jnp.sin(angles)
        cos_t = jnp.concatenate([cos_h, cos_h], axis=1)
        sin_t = jnp.concatenate([-sin_h, sin_h], axis=1)

        sds = jax.ShapeDtypeStruct
        tok = (SEQ, HD)
        q, k, v, qp, kp = call(
            proj_kernel, "proj", (NB,),
            [pl.BlockSpec((NG, 1, HD, DM), lambda t, ix: (t, ix[0], 0, 0)),
             pl.BlockSpec((NG, 1, HD, DM), lambda t, ix: (t, 0, 0, 0)),
             full((DM, HD)), full((DM, 256)), full((1, HD)), full((1, HD)), full(tok), full(tok)],
            [full_out(tok)] * 5,
            [sds(tok, BF16)] * 3 + [sds(tok, F32)] * 2, 2 * SEQ * DM * 384,
        )(idx, h_all, h_all, wq, wkv, gq, gk, cos_t, sin_t)

        o, lse = call(
            functools.partial(lambda ix, *a, scale: fwd_kernel(*a, scale=scale), scale=scale), "attn_fwd", (NB,),
            [pl.BlockSpec((BLK, HD), lambda t, ix: (t, 0)), full(tok), full(tok)],
            [full_out((ND, HD, HD)), full_out((NB, 1, BLK))],
            [sds((ND, HD, HD), BF16), sds((NB, 1, BLK), F32)], NG * SEQ * SEQ * HD,
            scratch=[pltpu.VMEM((HD, BLK), F32)],
        )(idx, q, k, v)
        o_tok = lax.all_to_all(o, 'cp', 0, 0)

        do = call(
            dout_kernel, "dout", (NB,),
            [pl.BlockSpec((NG, 1, HD, DM), lambda t, ix: (t, ix[0], 0, 0)), full((HD, DM))],
            full_out(tok), sds(tok, BF16), 2 * SEQ * DM * HD,
        )(idx, dy_all, wo)
        dwo = call(
            dwo_kernel, "dwo", (NB,),
            [pl.BlockSpec((NG, HD, HD), lambda t, ix: (t, 0, 0)),
             pl.BlockSpec((NG, 1, HD, DM), lambda t, ix: (t, ix[0], 0, 0))],
            full_out((HD, DM)), sds((HD, DM), F32), 2 * SEQ * DM * HD,
        )(idx, o, dy_all)
        dwo_all = lax.all_gather(dwo, 'cp')
        do, dwo = lax.optimization_barrier((do, dwo))

        dqp, dkv = call(
            functools.partial(bwd_kernel, scale=scale), "attn_bwd", (NB,),
            [full(tok), pl.BlockSpec((BLK, HD), lambda t, ix: (t, 0)), pl.BlockSpec((BLK, HD), lambda t, ix: (t, 0)),
             full(tok), full((ND, HD, HD)), full((NB, 1, BLK)), full(tok), full((1, HD)), full(tok), full(tok)],
            [full_out((ND, HD, HD)), full_out((2, 2, HALF, HD))],
            [sds((ND, HD, HD), BF16), sds((2, 2, HALF, HD), F32)], 10 * SEQ * SEQ * HD,
            scratch=[pltpu.VMEM((NB, HD, BLK), F32), pltpu.VMEM((BLK, HD), F32), pltpu.VMEM((BLK, HD), F32),
                     pltpu.VMEM((NB, 1, BLK), F32)],
        )(idx, q, k, v, do, o, lse, qp, gq, cos_t, sin_t)

        def dw_call(name, d_st, width, col, lay):
            return call(
                dwq_kernel, name, (NB,),
                [pl.BlockSpec((NG, 1, HD, width), lambda t, ix: (t, ix[0] if lay else 0, 0, 0 if width == DM else ix[0])),
                 pl.BlockSpec((NG, HD, HD), lambda t, ix: (t, 0, 0))],
                full_out((width, HD)), sds((width, HD), F32), 2 * SEQ * width * HD,
                scratch=[pltpu.VMEM((HD, width), F32)],
            )(idx, h_all, d_st)

        dwq = dw_call("dwq", dqp, DM, 0, True)
        dwq, dwo_all = lax.optimization_barrier((dwq, dwo_all))
        dwo_all = dwo_all.reshape(NB, 2, 256, DM)
        dwq_all = lax.all_gather(dwq, 'cp').reshape(NB, 2, 2, DM, HD)

        sum1 = dkv[0] + lax.ppermute(dkv[1], 'cp', core_perm)
        tot = sum1[0] + lax.ppermute(sum1[1], 'cp', layer_perm)
        half_at = (layer * HALF, 0)
        dk_proj = head_norm_rope_vjp(tot, lax.dynamic_slice(kp, half_at, (HALF, HD)), gk,
                                     lax.dynamic_slice(cos_t, half_at, (HALF, HD)),
                                     lax.dynamic_slice(sin_t, half_at, (HALF, HD)))
        mine = jnp.where(core == 0, dk_proj, tot).astype(BF16).reshape(ND, PC, HD)
        mine = jnp.where(is_a, mine, mine[::-1])
        other = lax.ppermute(mine, 'cp', layer_perm)
        d_kv_st = jnp.concatenate([jnp.where(is_a, mine, other), jnp.where(is_a, other, mine)], axis=1)

        back = lax.all_to_all(jnp.concatenate([dqp, mine], axis=1), 'cp', 0, 0).reshape(NB, 2, 2, 192, HD)
        dwkv = dw_call("dwkv", d_kv_st, BLK, 0, False)
        dwkv_all = lax.all_gather(dwkv, 'cp').reshape(NB, 2, 2, BLK, HD)

        o_tok = o_tok.reshape(NB, 2, 2, HD, HD)
        out_a = o_tok[:, 0].transpose(2, 0, 1, 3).reshape(HD, HALF)
        out_b = o_tok[:, 1].transpose(2, 0, 1, 3).reshape(HD, HALF)
        y_out_a = (x_in_a[0].astype(F32) + dot(out_a, w_oa, 1, 0)).astype(BF16)[None]
        y_out_b = (x_in_b[0].astype(F32) + dot(out_b, w_ob, 1, 0)).astype(BF16)[None]

        d_qa = back[:, 0, :, :HD].transpose(2, 0, 1, 3).reshape(HD, HALF)
        d_qb = back[:, 1, :, :HD].transpose(2, 0, 1, 3).reshape(HD, HALF)
        d_k = back[:, :, 0, HD:].transpose(1, 2, 0, 3).reshape(HD, DM)
        d_v = back[:, :, 1, HD:].transpose(1, 2, 0, 3).reshape(HD, DM)
        d_norm_a = dot(d_qa, w_qa, 1, 1) + dot(d_k, w_k, 1, 1) + dot(d_v, w_v, 1, 1)
        d_norm_b = dot(d_qb, w_qb, 1, 1)
        pull_na = jax.vjp(functools.partial(rms_norm, gain_vec=gain_in_a), x_in_a[0].astype(F32))[1]
        pull_nb = jax.vjp(functools.partial(rms_norm, gain_vec=gain_in_b), x_in_b[0].astype(F32))[1]
        dx_in_a = (dy_out_a[0].astype(F32) + pull_na(d_norm_a)[0]).astype(BF16)[None]
        dx_in_b = (dy_out_b[0].astype(F32) + pull_nb(d_norm_b)[0]).astype(BF16)[None]

        dw_oa = dwo_all[:, 0].reshape(HALF, DM)
        dw_ob = dwo_all[:, 1].reshape(HALF, DM)
        dw_qa = dwq_all[:, 0].transpose(2, 0, 1, 3).reshape(DM, HALF)
        dw_qb = dwq_all[:, 1].transpose(2, 0, 1, 3).reshape(DM, HALF)
        dw_k = dwkv_all[:, :, 0].transpose(1, 2, 0, 3).reshape(DM, DM)
        dw_v = dwkv_all[:, :, 1].transpose(1, 2, 0, 3).reshape(DM, DM)
        return y_out_a, y_out_b, dx_in_a, dx_in_b, dw_qa, dw_qb, dw_k, dw_v, dw_oa, dw_ob

    return jax.shard_map(local_fn, mesh=mesh, in_specs=(act_spec,) * NG + (rep_spec,) * 11, out_specs=(act_spec,) * NG + (rep_spec,) * 6, check_vma=False)
```
